128 devices in a mesh: row: 8 (over z_hi, y), col: 16 (over x, z_lo, core).
Axes of the slice: x: 4, y: 4, z: 4 (z_hi: 2, z_lo: 2; z = z_hi * 2 + z_lo), core: 2. Of those that a mesh axis runs over, the one named last changes fastest.
Arguments:
- noise: float32 [4096, 3072], P('row', 'col'), may hold values from -30 to 30
- images: float32 [12288, 3072], P('col', 'row'), may hold values from -6 to 6
- time_index: int32 [4096], P('row'), may hold values from 0 to 999
- w_in: float32 [3072, 3072], P(None, 'col'), may hold values from -0.109375 to 0.109375
- time_gain: float32 [3072], P('col'), may hold values from -5 to 5
- w_out: float32 [3072, 3072], P('col'), may hold values from -0.109375 to 0.109375
Outputs:
- targets: float32 [4096, 3072], P('row', 'col')
- row_pot: float32 [4096], P('row')
- col_pot: float32 [12288], P('col')
- grad_in: float32 [3072, 3072], P('row', 'col')
- grad_time: float32 [3072], P('col')
- grad_out: float32 [3072, 3072], P('col', 'row')
- mse: float32 [], replicated
The draws below stay inside these ranges and needn't reach their ends.
All inputs are finite; a program needn't handle non-finite values.
Results may differ from the reference program's by a relative error of at most 0.0003.
Values sent between devices are 32-bit elements; how exact they have to be, the bound alone decides.
No kernel may reach another device: no remote copies, remote signals or barrier semaphores. Data moves between devices by JAX's collectives and lax.ppermute only.
A program may use at most 128 MiB of HBM per device.

```python
import jax
import jax.numpy as jnp
from jax import lax

DIM = 3072
HID = 3072
ITERS = 2
TIMES = 1000
NOISE = 4096
IMAGES = 12288


def draw_noise(key, part):
    base = jax.random.normal(key, (NOISE, DIM), jnp.float32)
    return base


def place_ends(result, own_key, least, high):
    shape = result.shape
    spot = [jax.random.randint(jax.random.fold_in(own_key, axis), (), 0, shape[axis]) for axis in range(len(shape))]
    result = result.at[tuple(spot)].set(least)
    longest = shape.index(max(shape))
    spot[longest] = (spot[longest] + 1) % shape[longest]
    return result.at[tuple(spot)].set(high)


def block_scale(rng, extent, shards, low, top_value):
    factor_of, own = 1.0, jax.random.fold_in(rng, 6)
    for dim, blocks in shards:
        heights = jnp.exp(jax.random.uniform(jax.random.fold_in(own, dim), (blocks,), jnp.float32, low / len(shards), top_value / len(shards)))
        factor_of = factor_of * jnp.repeat(heights, extent[dim] // blocks).reshape([-1 if axis == dim else 1 for axis in range(len(extent))])
    return factor_of


def bell_draw(key, dims, width, bound, split=(), dtype=jnp.bfloat16):
    gain = block_scale(key, dims, split, -0.22, 0.18) if split else 1.0
    drawn = jax.random.normal(key, dims, jnp.float32) * width * gain
    return jnp.minimum(jnp.maximum(drawn, -bound), bound).astype(dtype)


def setup_inputs(seed: int = 0) -> dict:
    key_of = jax.random.split(jax.random.key(seed), 7)
    noise = draw_noise(jax.random.fold_in(key_of[6], 71), 0)
    images = bell_draw(key_of[1], (IMAGES, DIM), 1.0, 6.0, ((0, 16), (1, 8)), jnp.float32)
    time_index = place_ends(jax.random.randint(key_of[2], (NOISE,), 0, TIMES), jax.random.fold_in(key_of[2], 1), 0, TIMES - 1).astype(jnp.int32)
    w_in = bell_draw(key_of[3], (DIM, HID), DIM ** -0.5, 0.109375, ((1, 16),), jnp.float32)
    time_gain = bell_draw(key_of[4], (HID,), 1.0, 5.0, ((0, 16),), jnp.float32)
    w_out = bell_draw(key_of[5], (HID, DIM), HID ** -0.5, 0.109375, ((0, 16),), jnp.float32)
    return dict(noise=noise, images=images, time_index=time_index, w_in=w_in, time_gain=time_gain, w_out=w_out)


EPSILON = 0.01

def log_sum_exp(values, axis):
    peak = lax.optimization_barrier(jnp.max(values, axis=axis, keepdims=True))
    total = lax.optimization_barrier(jnp.sum(jnp.exp(values - peak), axis=axis, keepdims=True))
    return jnp.squeeze(jnp.log(total) + peak, axis=axis)

def reference(noise, images, time_index, w_in, time_gain, w_out):
    highest = lax.Precision.HIGHEST
    noise_norms = lax.optimization_barrier(jnp.sum(noise * noise, axis=1))
    image_norms = lax.optimization_barrier(jnp.sum(images * images, axis=1))
    cross = jnp.dot(noise, images.T, precision=highest, preferred_element_type=jnp.float32)
    scaled = (noise_norms[:, None] + image_norms[None, :] - 2.0 * cross) / (DIM * EPSILON)
    col_pot = jnp.zeros((IMAGES,), jnp.float32)
    row_pot = jnp.zeros((NOISE,), jnp.float32)
    for iteration in range(ITERS):
        row_pot = jnp.log(jnp.float32(IMAGES)) - log_sum_exp(col_pot[None, :] - scaled, 1)
        col_pot = jnp.log(jnp.float32(NOISE)) - log_sum_exp(row_pot[:, None] - scaled, 0)
    logits = col_pot[None, :] - scaled
    weights = jnp.exp(logits - log_sum_exp(logits, 1)[:, None])
    targets = jnp.dot(weights, images, precision=highest, preferred_element_type=jnp.float32)
    fraction = (time_index.astype(jnp.float32) + 0.5) / TIMES
    mixed = (1.0 - fraction)[:, None] * noise + fraction[:, None] * targets
    velocity = targets - noise
    pre = jnp.dot(mixed, w_in, precision=highest, preferred_element_type=jnp.float32) + fraction[:, None] * time_gain[None, :]
    sigma = jax.nn.sigmoid(pre)
    hidden = pre * sigma
    out = jnp.dot(hidden, w_out, precision=highest, preferred_element_type=jnp.float32)
    diff = out - velocity
    mse = jnp.sum(diff * diff) / (NOISE * DIM)
    slope = diff / jnp.sqrt(jnp.float32(NOISE))
    grad_out = jnp.dot(hidden.T, slope, precision=highest, preferred_element_type=jnp.float32)
    back = jnp.dot(slope, w_out.T, precision=highest, preferred_element_type=jnp.float32)
    dpre = back * sigma * (1.0 + pre * (1.0 - sigma))
    grad_in = jnp.dot(mixed.T, dpre, precision=highest, preferred_element_type=jnp.float32)
    grad_time = lax.optimization_barrier(jnp.sum(fraction[:, None] * dpre, axis=0))
    return (targets, row_pot, col_pot, grad_in, grad_time, grad_out, mse)
```

```python
import jax
import jax.numpy as jnp
from jax import lax
from jax.sharding import Mesh
from jax.sharding import PartitionSpec as P


ITERS = 2
TIMES = 1000
ROW = ("zh", "y")
COL = ("x", "zl", "c")
EPSILON = 0.01
PRECISION = lax.Precision.HIGH


def dot(a, b, ca, cb):
    return lax.dot_general(
        a,
        b,
        (((ca,), (cb,)), ((), ())),
        precision=PRECISION,
        preferred_element_type=jnp.float32,
    )


def moved(array, steps):
    axes = tuple(steps)
    sizes = [lax.axis_size(axis) for axis in axes]
    total = 1
    for size in sizes:
        total *= size
    pairs = []
    for source in range(total):
        rest, place, weight = source, 0, 1
        for axis, size in zip(reversed(axes), reversed(sizes)):
            place += (rest % size + steps[axis]) % size * weight
            weight, rest = weight * size, rest // size
        pairs.append((source, place))
    return lax.ppermute(array, axes if len(axes) > 1 else axes[0], pairs)


def around(array, ring, pair, far_by_pair=False):
    half = array.shape[0] // 2
    far = moved(array, {pair: 1})
    got = {(0, 0): array, (0, 1): far}
    for flip, own in ((0, array), (1, far)):
        got[1, flip] = moved(own, {ring: 1})
        got[3, flip] = moved(own, {ring: -1})
        if not far_by_pair:
            near = (3, -1) if flip else (1, 1)
            got[2, flip] = moved(got[near[0], flip], {ring: near[1]})
        elif flip:
            got[2, 1] = moved(got[2, 0], {pair: 1})
        else:
            right = moved(got[1, 0][:half], {ring: 1})
            left = moved(got[3, 0][half:], {ring: -1})
            got[2, 0] = jnp.concatenate([right, left])
    return got


def placed(got, ring, pair):
    buffer = jnp.zeros((8, *got[0, 0].shape), got[0, 0].dtype)
    here, side = lax.axis_index(ring), lax.axis_index(pair)
    for (step, flip), chunk in got.items():
        place = (here - step) % 4 * 2 + (side + flip) % 2
        buffer = lax.dynamic_update_index_in_dim(buffer, chunk, place, 0)
    return buffer


def gathered(chunk):
    return placed(around(chunk, "x", "zl"), "x", "zl").reshape(-1, chunk.shape[1])


def scattered(parts, ring, pair):
    right = moved(parts[2][0], {ring: 1})
    left = moved(parts[2][1], {ring: -1})
    a1 = moved(parts[1][1], {ring: 1})
    b0 = moved(parts[3][0], {ring: -1})
    a0 = moved(parts[1][0] + right, {ring: 1})
    b1 = moved(parts[3][1] + left, {ring: -1})
    second = [[a0, a1], [b0, b1]]
    mine = [parts[0][k] + second[0][k] + second[1][k] for k in (0, 1)]
    first = lax.axis_index(pair) == 0
    keep = jnp.where(first, mine[0], mine[1])
    send = jnp.where(first, mine[1], mine[0])
    return keep + moved(send, {pair: 1})


def both_cores(array, dim=0):
    other = moved(array, {"c": 1})
    first = lax.axis_index("c") == 0
    return jnp.concatenate([jnp.where(first, array, other), jnp.where(first, other, array)], dim)


def own_half(array, dim):
    low, high = jnp.split(array, 2, dim)
    first = lax.axis_index("c") == 0
    return jnp.where(first, low, high), jnp.where(first, high, low)


def turned(array, dim):
    own, other = own_half(array, dim)
    return jnp.concatenate([own, other], dim)


def joined(pieces):
    peaks = jnp.stack([piece[0] for piece in pieces])
    totals = jnp.stack([piece[1] for piece in pieces])
    peak = jnp.max(peaks, 0)
    return jnp.stack([peak, jnp.sum(totals * jnp.exp(peaks - peak), 0)])


def swapped(piece):
    low, high = jnp.split(piece, 2, 1)
    return jnp.concatenate([high, low], 1)


def over_images(logits):
    peak = jnp.max(logits, 0)
    both = jnp.stack([peak, jnp.sum(jnp.exp(logits - peak), 0)])
    both = joined(
        [
            both,
            moved(both, {"zl": 1}),
            swapped(moved(both, {"c": 1})),
            swapped(moved(both, {"zl": 1, "c": 1})),
        ]
    )
    both = joined([both] + [moved(both, {"x": step}) for step in (1, 2, 3)])
    return jnp.log(both[1]) + both[0]


def over_noise(logits):
    peak = jnp.max(logits, 1)
    both = jnp.stack([peak, jnp.sum(jnp.exp(logits - peak[:, None]), 1)])
    both = joined([both, moved(both, {"zh": 1})])
    both = joined([both] + [moved(both, {"y": step}) for step in (1, 2, 3)])
    return jnp.log(both[1]) + both[0]


def body(noise, images, time_index, w_in, time_gain, w_out):
    x, zl, c = (lax.axis_index(axis) for axis in COL)
    zh, y = (lax.axis_index(axis) for axis in ROW)
    width = noise.shape[1] * lax.axis_size(COL)
    noise_count = noise.shape[0] * lax.axis_size(ROW)
    image_count = images.shape[0] * lax.axis_size(COL)

    keep, send = own_half(noise.T, 1)
    got = moved(send, {"c": 1})
    own_noise = jnp.where(c == 0, jnp.concatenate([keep, got]), jnp.concatenate([got, keep]))
    half_noise = gathered(own_noise)
    full_noise = jnp.concatenate([half_noise, moved(half_noise, {"c": 1})], 1)
    depth = own_noise.shape[0]

    pieces = around(images, "y", "zh", True)
    image_at = jnp.stack([pieces[step, flip] for step in range(4) for flip in range(2)])
    cross, image_norms = 0.0, 0.0
    for step, flip in ((0, 0), (1, 0), (3, 0), (0, 1), (2, 0), (1, 1), (3, 1), (2, 1)):
        piece = pieces[step, flip]
        place = (zh + flip) % 2 * 4 + (y - step) % 4
        block = lax.dynamic_slice_in_dim(full_noise, place * depth, depth, 0)
        cross = lax.optimization_barrier(cross + dot(piece, block, 1, 0))
        image_norms = image_norms + jnp.sum(piece * piece, 1)
    noise_norms = jnp.sum(full_noise * full_noise, 0)
    scaled = (noise_norms[None, :] + image_norms[:, None] - 2.0 * cross) / (width * EPSILON)

    chip_in = both_cores(w_in.T)
    chip_out = both_cores(w_out)
    chip_gain = both_cores(time_gain)
    lines = jnp.zeros((4, w_out.shape[0], 2 * depth), w_out.dtype)
    for step in (0, 1, 3, 2):
        to = (x + step) % 4 * 2
        block = lax.dynamic_slice_in_dim(w_out, to * depth, 2 * depth, 1)
        if step:
            block = moved(block, {"x": step})
        lines = lax.dynamic_update_index_in_dim(lines, block, (x - step) % 4, 0)
    low, high = jnp.split(lines, 2, 2)
    keep = jnp.where(zl == 0, low, high)
    got = moved(jnp.where(zl == 0, high, low), {"zl": 1})
    columns = jnp.where(zl == 0, jnp.stack([keep, got], 1), jnp.stack([got, keep], 1))
    columns = both_cores(columns[:, :, None], 2).reshape(-1, depth)

    col_pot = jnp.zeros((images.shape[0],), jnp.float32)
    for _ in range(ITERS):
        row_pot = jnp.log(jnp.float32(image_count)) - over_images(col_pot[:, None] - scaled)
        col_pot = jnp.log(jnp.float32(noise_count)) - over_noise(row_pot[None, :] - scaled)
    logits = col_pot[:, None] - scaled
    weights = jnp.exp(logits - over_images(logits)[None, :])

    parts = {step: [None, None] for step in range(4)}
    for step, side in ((2, 0), (2, 1), (1, 1), (3, 0), (1, 0), (3, 1), (0, 0), (0, 1)):
        place = (x + step) % 4 * 2 + side
        place = (y - place) % 4 * 2 + (zh + place // 4) % 2
        block = lax.dynamic_index_in_dim(image_at, place, 0, False)
        part = dot(block, weights, 0, 0)
        own, other = jnp.split(part, 2, 1)
        parts[step][side] = own + moved(other, {"c": 1})
    own_targets = scattered(parts, "x", "zl")

    keep, send = own_half(own_targets, 0)
    targets = turned(jnp.concatenate([keep, moved(send, {"c": 1})], 1), 1).T

    fraction = (time_index.astype(jnp.float32) + 0.5) / TIMES
    fraction = own_half(fraction, 0)[0]
    mixed = (1.0 - fraction) * own_noise + fraction * own_targets
    all_mixed = gathered(mixed)
    pre = dot(chip_in, all_mixed, 1, 0) + chip_gain[:, None] * fraction
    sigma = jax.nn.sigmoid(pre)
    hidden = pre * sigma
    all_hidden = gathered(hidden)
    out = dot(columns, all_hidden, 0, 0)
    diff = out - (own_targets - own_noise)
    slope = diff / jnp.sqrt(jnp.float32(noise_count))
    all_slope = gathered(slope)
    squared = jnp.sum(all_slope * all_slope) * noise_count

    def whole(array):
        keep, send = own_half(array, 0)
        return jnp.concatenate([keep, moved(send, {"c": 1})], 1)

    def gradient(left, right):
        right = jnp.concatenate([right, moved(right, {"c": 1})], 1)
        parts = {step: [None, None] for step in range(4)}
        for step, side in ((2, 0), (2, 1), (1, 1), (3, 0), (1, 0), (3, 1), (0, 0), (0, 1)):
            place = side * 4 + (y + step) % 4
            block = lax.dynamic_slice_in_dim(right, place * depth, depth, 0)
            parts[step][side] = dot(left, block, 1, 1)
        return scattered(parts, "y", "zh")

    grad_out = gradient(whole(hidden), all_slope)
    back = dot(chip_out, all_slope, 1, 0)
    dpre = back * sigma * (1.0 + pre * (1.0 - sigma))
    grad_in = gradient(whole(dpre), all_mixed).T

    sums = jnp.concatenate([jnp.sum(fraction * dpre, 1), squared[None]])
    sums = jnp.pad(sums, (0, -len(sums) % 128))
    sums = sums + moved(sums, {"c": 1})
    sums = sums + moved(sums, {"zh": 1})
    sums = sums + (moved(sums, {"y": 1}) + moved(sums, {"y": 2}) + moved(sums, {"y": 3}))
    grad_time = own_half(sums[: 2 * w_in.shape[1]], 0)[0]
    mse = sums[2 * w_in.shape[1]] / (noise_count * width)
    return (targets, turned(row_pot, 0), col_pot, grad_in, grad_time, grad_out, mse)


def solution(mesh):
    torus = Mesh(mesh.devices.reshape(2, 4, 4, 2, 2), (*ROW, *COL))
    return jax.shard_map(
        body,
        mesh=torus,
        in_specs=(P(ROW, COL), P(COL, ROW), P(ROW), P(None, COL), P(COL), P(COL, None)),
        out_specs=(P(ROW, COL), P(ROW), P(COL), P(ROW, COL), P(COL), P(COL, ROW), P()),
        check_vma=False,
    )
```
